32 devices in a mesh: data: 2 (over x), time: 16 (over z, y, core).
Axes of the slice: x: 2, y: 2, z: 4, core: 2. Of those that a mesh axis runs over, the one named last changes fastest.
Arguments:
- x_init: float32 [24, 256, 384], P('data'), parts along dimension 0
- w_in: bfloat16 [384, 1536], replicated
- w_out: bfloat16 [1536, 384], replicated
- mod_gamma: bfloat16 [64, 1536], P('time')
- mod_beta: bfloat16 [64, 1536], P('time')
- step_size: float32 [64], P('time')
Outputs:
- output: float32 [24, 256, 384], P('data'), parts along dimension 0
There are 2 independent parts. The reference program is written for one: setup_inputs(seed, part) draws one part's arguments, and reference() takes and returns one part's arrays. A program takes and returns all parts, laid end to end along the dimension named above; an argument that names none is the same for every part.
All inputs are finite; a program needn't handle non-finite values.
Results may differ from the reference program's by a relative error of at most 0.001.
Values are sent between devices in bfloat16 or wider.
A program may use at most 1 GiB of HBM per device.

```python
import jax
import jax.numpy as jnp
from jax import lax

SAMPLES = 12
TOKENS = 256
CHANNELS = 384
HIDDEN = 1536
NUM_STEPS = 64
SWEEPS = 4


def setup_inputs(seed: int = 0, part: int = 0) -> dict:
    base_key = jax.random.key(seed)
    part_key = jax.random.fold_in(base_key, part)
    sub_keys = jax.random.split(base_key, 6)
    x_init = jax.random.normal(part_key, (SAMPLES, TOKENS, CHANNELS), jnp.float32)
    w_in = (jax.random.normal(sub_keys[0], (CHANNELS, HIDDEN), jnp.float32) * CHANNELS ** -0.5).astype(jnp.bfloat16)
    w_out = (jax.random.normal(sub_keys[1], (HIDDEN, CHANNELS), jnp.float32) * HIDDEN ** -0.5).astype(jnp.bfloat16)
    mod_gamma = (0.5 * jax.random.normal(sub_keys[2], (NUM_STEPS, HIDDEN), jnp.float32)).astype(jnp.bfloat16)
    mod_beta = jax.random.normal(sub_keys[3], (NUM_STEPS, HIDDEN), jnp.float32).astype(jnp.bfloat16)
    total_time = 1.0 + 2.0 * jax.random.uniform(sub_keys[4], (), jnp.float32)
    step_size = (0.5 + jax.random.uniform(sub_keys[5], (NUM_STEPS,), jnp.float32)) * (total_time / NUM_STEPS)
    return {"x_init": x_init, "w_in": w_in, "w_out": w_out, "mod_gamma": mod_gamma, "mod_beta": mod_beta, "step_size": step_size}


def drift_of(latents, w_in, w_out, gamma_j, beta_j, h_step):
    pre_act = jnp.dot(latents.astype(jnp.bfloat16).reshape(-1, CHANNELS), w_in, preferred_element_type=jnp.float32)
    hidden_act = jax.nn.gelu(pre_act * (1.0 + gamma_j.astype(jnp.float32)) + beta_j.astype(jnp.float32), approximate=True).astype(jnp.bfloat16)
    proj_out = jnp.dot(hidden_act, w_out, preferred_element_type=jnp.float32)
    return h_step * proj_out.reshape(latents.shape)


def reference(x_init, w_in, w_out, mod_gamma, mod_beta, step_size):
    run_init = jnp.zeros((SWEEPS,) + x_init.shape, jnp.float32)

    def step_body(run_sums, step_in):
        gamma_j, beta_j, h_step = step_in
        latents = jnp.concatenate([x_init[None], x_init[None] + run_sums[:-1]], axis=0)
        return run_sums + drift_of(latents, w_in, w_out, gamma_j, beta_j, h_step), None

    run_sums, _ = lax.scan(step_body, run_init, (mod_gamma, mod_beta, step_size))
    return x_init + run_sums[-1]
```

```python
import functools
import math

import jax
import jax.numpy as jnp
from jax import lax
from jax.experimental import pallas as pl
from jax.experimental.pallas import tpu as pltpu
from jax.sharding import PartitionSpec as P

PASSES = 2
OWN = 4
DEVS = 16
STEPS = OWN * DEVS
BLOCKS = DEVS + -(-3 // OWN)
TILE = 256
C0 = math.sqrt(2.0 / math.pi)
K0 = 2.0 * C0
K1 = 8.0 * C0 * 0.044715


def _sampler(x_ref, win_ref, wout_ref, gam_ref, bet_ref, h_ref, y_ref,
             x_s, gam_all, bet_all, h_all, scale, shift, h_row, a0, run, total,
             xb, hid, y_all,
             x_sem, out_sem, ms, mr, zs, zr, ys, yr, cs, cr):
    every = x_s.shape[0]
    first = every * 2 // 3
    spans = ((0, first), (first, every - first))
    hidden = a0.shape[1]
    tiles = [pl.ds(i * TILE, TILE) for i in range(hidden // TILE)]
    me = lax.axis_index("time")
    z = me // 4
    y = (me // 2) % 2
    c = me % 2

    def dev(zz, yy, cc):
        return zz * 4 + yy * 2 + cc

    barrier = pltpu.get_barrier_semaphore()
    for d in range(1, DEVS):
        pl.semaphore_signal(barrier, inc=1, device_id={"time": lax.rem(me + d, DEVS)},
                            device_id_type=pl.DeviceIdType.MESH)
    x_copy = pltpu.make_async_copy(
        x_ref.at[me], x_s, x_sem)
    x_copy.start()
    gam_all[me] = gam_ref[...]
    bet_all[me] = bet_ref[...]
    h_all[me] = h_ref[...]
    pl.semaphore_wait(barrier, DEVS - 1)

    def mod_copies(d, owner, peer):
        pairs = ((gam_ref, gam_all), (bet_ref, bet_all), (h_ref, h_all))
        return [pltpu.make_async_remote_copy(
            src_ref=src, dst_ref=dst.at[owner], send_sem=ms.at[d, i],
            recv_sem=mr.at[owner, i], device_id={"time": peer},
            device_id_type=pl.DeviceIdType.MESH)
            for i, (src, dst) in enumerate(pairs)]

    def send_mods():
        def one(d, carry):
            for copy in mod_copies(d, me, lax.rem(me + d, DEVS)):
                copy.start()
            return carry
        lax.fori_loop(1, DEVS, one, 0)

    def take_mods(b):
        @pl.when(b != me)
        def _():
            for copy in mod_copies(0, b, me):
                copy.wait_recv()
        for k in range(OWN):
            scale[b * OWN + k] = 0.5 * (1.0 + gam_all[b, k:k + 1, :].astype(jnp.float32))
            shift[b * OWN + k] = 0.5 * bet_all[b, k:k + 1, :].astype(jnp.float32)
            h_row[b * OWN + k] = h_all[b, k:k + 1, :]

    def block_copy(p, block, peer, send, recv):
        span = pl.ds(*spans[p])
        return pltpu.make_async_remote_copy(
            src_ref=y_all.at[block, span], dst_ref=y_all.at[block, span],
            send_sem=send, recv_sem=recv, device_id={"time": peer},
            device_id_type=pl.DeviceIdType.MESH)

    def z_send(p, d):
        return block_copy(p, me, dev(lax.rem(z + d, 4), y, c), zs.at[p, d - 1], zr.at[p, d - 1])

    def z_recv(p, d):
        return block_copy(p, dev(lax.rem(z + 4 - d, 4), y, c), me, zs.at[p, d - 1], zr.at[p, d - 1])

    def y_send(p, k):
        return block_copy(p, dev(lax.rem(z + 4 - k, 4), y, c), dev(z, 1 - y, c), ys.at[p, k], yr.at[p, k])

    def y_recv(p, k):
        return block_copy(p, dev(lax.rem(z + 4 - k, 4), 1 - y, c), me, ys.at[p, k], yr.at[p, k])

    def c_block(k, cc):
        yy = y if k < 4 else 1 - y
        return dev(lax.rem(z + 4 - k % 4, 4), yy, cc)

    def c_send(p, k):
        return block_copy(p, c_block(k, c), dev(z, y, 1 - c), cs.at[p, k], cr.at[p, k])

    def c_recv(p, k):
        return block_copy(p, c_block(k, 1 - c), me, cs.at[p, k], cr.at[p, k])

    def gather_first(p):
        for d in (1, 3, 2):
            z_send(p, d).start()
        y_send(p, 0).start()
        c_send(p, 0).start()

    def gather_second(p):
        for d in (1, 3, 2):
            z_recv(p, d).wait_recv()
            y_send(p, d).start()
            c_send(p, d).start()

    def gather_third(p):
        for k in (0, 1, 3, 2):
            y_recv(p, k).wait_recv()
            c_send(p, 4 + k).start()

    def out_copy(p):
        span = pl.ds(*spans[p])
        return pltpu.make_async_copy(y_all.at[:, span], y_ref.at[:, span], out_sem.at[p])

    def gather_last(p):
        for k in range(8):
            c_recv(p, k).wait_recv()
        out_copy(p).start()

    @pl.when(me < 2)
    def _():
        send_mods()

    x_copy.wait()

    def body(p, n):
        rows = spans[p][1]
        x0 = x_s[pl.ds(*spans[p])]
        for s in range(3):
            xb[s * rows:(s + 1) * rows, :] = (x0 + run[s, 0:rows]).astype(jnp.bfloat16)
        acc = None
        steps = [n - s for s in range(4)]
        index = [jnp.clip(j, 0, STEPS - 1) for j in steps]
        for t in tiles:
            part = jnp.dot(hid[0:3 * rows, t], wout_ref[t, :], preferred_element_type=jnp.float32)
            acc = part if acc is None else acc + part
            pre = jnp.dot(xb[0:3 * rows, :], win_ref[:, t], preferred_element_type=jnp.float32)
            for s in range(4):
                a = a0[0:rows, t] if s == 0 else pre[(s - 1) * rows:s * rows, :]
                v = a * scale[index[s], :, t] + shift[index[s], :, t]
                g = (v + v * jnp.tanh(v * (K1 * (v * v) + K0))).astype(jnp.bfloat16)
                if s < 3:
                    hid[s * rows:(s + 1) * rows, t] = g
                else:
                    term = h_row[index[s], :, 0:TILE] * g.astype(jnp.float32)
                    good = jnp.logical_and(steps[s] >= 0, steps[s] < STEPS)
                    total[0:rows, t] += jnp.where(good, term, 0.0)
        for s in range(3):
            j = n - 1 - s
            good = jnp.logical_and(j >= 0, j < STEPS)
            term = h_row[jnp.clip(j, 0, STEPS - 1)] * acc[s * rows:(s + 1) * rows, :]
            run[s, 0:rows] = run[s, 0:rows] + jnp.where(good, term, 0.0)

    for p in range(PASSES):
        rows = spans[p][1]
        run[...] = jnp.zeros_like(run)
        total[...] = jnp.zeros_like(total)
        hid[...] = jnp.zeros_like(hid)
        xb[0:rows, :] = x_s[pl.ds(*spans[p])].astype(jnp.bfloat16)
        for t in tiles:
            a0[0:rows, t] = jnp.dot(xb[0:rows, :], win_ref[:, t], preferred_element_type=jnp.float32)

        def block(b, carry, p=p):
            if p == 0:
                @pl.when(b + 2 == me)
                def _():
                    send_mods()

                @pl.when(b < DEVS)
                def _():
                    take_mods(b)
            else:
                for at, stage in ((7, gather_second), (13, gather_third), (16, gather_last)):
                    @pl.when(b == at)
                    def _(stage=stage):
                        stage(p - 1)

            def inner(k, carry):
                body(p, b * OWN + k)
                return carry
            lax.fori_loop(0, OWN, inner, 0, unroll=OWN)
            return carry

        lax.fori_loop(0, BLOCKS, block, 0)

        for t in tiles:
            rest = total[0:rows, t]
            for s in range(3):
                part = rest.astype(jnp.bfloat16)
                hid[s * rows:(s + 1) * rows, t] = part
                rest = rest - part.astype(jnp.float32)
        out = jnp.dot(hid[0:3 * rows, :], wout_ref[...], preferred_element_type=jnp.float32)
        out = out[0:rows] + (out[rows:2 * rows] + out[2 * rows:3 * rows])
        y_all[me, pl.ds(*spans[p])] = x_s[pl.ds(*spans[p])] + out
        gather_first(p)

    last = PASSES - 1
    gather_second(last)
    gather_third(last)
    gather_last(last)
    for p in range(PASSES):
        for d in range(1, 4):
            z_send(p, d).wait_send()
        for k in range(4):
            y_send(p, k).wait_send()
        for k in range(8):
            c_send(p, k).wait_send()

    def sent(d, carry):
        for copy in mod_copies(d, me, lax.rem(me + d, DEVS)):
            copy.wait_send()
        return carry
    lax.fori_loop(1, DEVS, sent, 0)
    for p in range(PASSES):
        out_copy(p).wait()


def solution(mesh):
    assert mesh.shape["time"] == DEVS

    def local_run(x_init, w_in, w_out, mod_gamma, mod_beta, step_size):
        channels, hidden = w_in.shape
        every = x_init.size // channels // DEVS
        rows = every * 2 // 3
        x_rows = x_init.reshape(DEVS, every, channels)
        h_wide = jnp.broadcast_to(step_size[:, None], (OWN, channels))
        vmem = pl.BlockSpec(memory_space=pltpu.VMEM)
        dma = pltpu.SemaphoreType.DMA
        f32, bf16 = jnp.float32, jnp.bfloat16
        y = pl.pallas_call(
            _sampler,
            out_shape=jax.ShapeDtypeStruct((DEVS, every, channels), f32),
            in_specs=[pl.BlockSpec(memory_space=pl.ANY)] + [vmem] * 5,
            out_specs=pl.BlockSpec(memory_space=pl.ANY),
            scratch_shapes=[
                pltpu.VMEM((every, channels), f32),
                pltpu.VMEM((DEVS, OWN, hidden), bf16),
                pltpu.VMEM((DEVS, OWN, hidden), bf16),
                pltpu.VMEM((DEVS, OWN, channels), f32),
                pltpu.VMEM((STEPS, 1, hidden), f32),
                pltpu.VMEM((STEPS, 1, hidden), f32),
                pltpu.VMEM((STEPS, 1, channels), f32),
                pltpu.VMEM((rows, hidden), f32),
                pltpu.VMEM((3, rows, channels), f32),
                pltpu.VMEM((rows, hidden), f32),
                pltpu.VMEM((3 * rows, channels), bf16),
                pltpu.VMEM((3 * rows, hidden), bf16),
                pltpu.VMEM((DEVS, every, channels), f32),
                dma(()), dma((PASSES,)),
                dma((DEVS, 3)), dma((DEVS, 3)),
                dma((PASSES, 3)), dma((PASSES, 3)),
                dma((PASSES, 4)), dma((PASSES, 4)),
                dma((PASSES, 8)), dma((PASSES, 8)),
            ],
            compiler_params=pltpu.CompilerParams(
                collective_id=0, has_side_effects=True, vmem_limit_bytes=48 * 1024 * 1024),
            name="sampler",
        )(x_rows, w_in, w_out, mod_gamma, mod_beta, h_wide)
        return y.reshape(x_init.shape)

    return jax.shard_map(
        local_run, mesh=mesh,
        in_specs=(P("data", None, None), P(None, None), P(None, None),
                  P("time", None), P("time", None), P("time")),
        out_specs=P("data", None, None), check_vma=False)
```

```python
import functools
import math

import jax
import jax.numpy as jnp
from jax import lax
from jax.experimental import pallas as pl
from jax.experimental.pallas import tpu as pltpu
from jax.sharding import PartitionSpec as P

PASSES = 2
OWN = 4
DEVS = 16
STEPS = OWN * DEVS
TILE = 256
C0 = math.sqrt(2.0 / math.pi)
K0 = 2.0 * C0
K1 = 8.0 * C0 * 0.044715


def _sampler(x_ref, win_hbm, wout_hbm, gam_ref, bet_ref, h_ref, y_ref,
             win_ref, wout_ref, x_s, gam_all, bet_all, h_all, scale, shift, h_row, a0, run, total,
             xb, hid, y_all,
             x_sem, w_sem, out_sem, ms, mr, zs, zr, ys, yr, cs, cr):
    every = x_s.shape[0]
    first = every * 2 // 3
    spans = ((0, first), (first, every - first))
    hidden = a0.shape[1]
    tiles = [pl.ds(i * TILE, TILE) for i in range(hidden // TILE)]
    me = lax.axis_index("time")
    z = me // 4
    y = (me // 2) % 2
    c = me % 2

    def dev(zz, yy, cc):
        return zz * 4 + yy * 2 + cc

    barrier = pltpu.get_barrier_semaphore()
    for d in range(1, DEVS):
        pl.semaphore_signal(barrier, inc=1, device_id={"time": lax.rem(me + d, DEVS)},
                            device_id_type=pl.DeviceIdType.MESH)
    x_copy = pltpu.make_async_copy(
        x_ref.at[me], x_s, x_sem)
    x_copy.start()
    w_copies = [pltpu.make_async_copy(src, dst, w_sem.at[i]) for i, (src, dst) in
                enumerate(((win_hbm, win_ref), (wout_hbm, wout_ref)))]
    for copy in w_copies:
        copy.start()
    gam_all[me] = gam_ref[...]
    bet_all[me] = bet_ref[...]
    h_all[me] = h_ref[...]
    pl.semaphore_wait(barrier, DEVS - 1)

    def mod_copies(d, owner, peer):
        pairs = ((gam_ref, gam_all), (bet_ref, bet_all), (h_ref, h_all))
        return [pltpu.make_async_remote_copy(
            src_ref=src, dst_ref=dst.at[owner], send_sem=ms.at[d, i],
            recv_sem=mr.at[owner, i], device_id={"time": peer},
            device_id_type=pl.DeviceIdType.MESH)
            for i, (src, dst) in enumerate(pairs)]

    def send_mods():
        def one(d, carry):
            for copy in mod_copies(d, me, lax.rem(me + d, DEVS)):
                copy.start()
            return carry
        lax.fori_loop(1, DEVS, one, 0)

    def take_mods(b):
        @pl.when(b != me)
        def _():
            for copy in mod_copies(0, b, me):
                copy.wait_recv()
        for k in range(OWN):
            scale[b * OWN + k] = 0.5 * (1.0 + gam_all[b, k:k + 1, :].astype(jnp.float32))
            shift[b * OWN + k] = 0.5 * bet_all[b, k:k + 1, :].astype(jnp.float32)
            h_row[b * OWN + k] = h_all[b, k:k + 1, :]

    def block_copy(p, block, peer, send, recv):
        span = pl.ds(*spans[p])
        return pltpu.make_async_remote_copy(
            src_ref=y_all.at[block, span], dst_ref=y_all.at[block, span],
            send_sem=send, recv_sem=recv, device_id={"time": peer},
            device_id_type=pl.DeviceIdType.MESH)

    def z_send(p, d):
        return block_copy(p, me, dev(lax.rem(z + d, 4), y, c), zs.at[p, d - 1], zr.at[p, d - 1])

    def z_recv(p, d):
        return block_copy(p, dev(lax.rem(z + 4 - d, 4), y, c), me, zs.at[p, d - 1], zr.at[p, d - 1])

    def y_send(p, k):
        return block_copy(p, dev(lax.rem(z + 4 - k, 4), y, c), dev(z, 1 - y, c), ys.at[p, k], yr.at[p, k])

    def y_recv(p, k):
        return block_copy(p, dev(lax.rem(z + 4 - k, 4), 1 - y, c), me, ys.at[p, k], yr.at[p, k])

    def c_block(k, cc):
        yy = y if k < 4 else 1 - y
        return dev(lax.rem(z + 4 - k % 4, 4), yy, cc)

    def c_send(p, k):
        return block_copy(p, c_block(k, c), dev(z, y, 1 - c), cs.at[p, k], cr.at[p, k])

    def c_recv(p, k):
        return block_copy(p, c_block(k, 1 - c), me, cs.at[p, k], cr.at[p, k])

    def gather_first(p):
        for d in (1, 3, 2):
            z_send(p, d).start()
        y_send(p, 0).start()
        c_send(p, 0).start()

    def gather_second(p):
        for d in (1, 3, 2):
            z_recv(p, d).wait_recv()
            y_send(p, d).start()
            c_send(p, d).start()

    def gather_third(p):
        for k in (0, 1, 3, 2):
            y_recv(p, k).wait_recv()
            c_send(p, 4 + k).start()

    def out_copy(p):
        span = pl.ds(*spans[p])
        return pltpu.make_async_copy(y_all.at[:, span], y_ref.at[:, span], out_sem.at[p])

    def gather_last(p):
        for k in range(8):
            c_recv(p, k).wait_recv()
        out_copy(p).start()

    @pl.when(me < 2)
    def _():
        send_mods()

    x_copy.wait()
    for copy in w_copies:
        copy.wait()

    def body(p, n):
        rows = spans[p][1]
        x0 = x_s[pl.ds(*spans[p])]
        for s in range(3):
            xb[s * rows:(s + 1) * rows, :] = (x0 + run[s, 0:rows]).astype(jnp.bfloat16)
        acc = None
        steps = [n - s for s in range(4)]
        index = [jnp.clip(j, 0, STEPS - 1) for j in steps]
        for t in tiles:
            part = jnp.dot(hid[0:3 * rows, t], wout_ref[t, :], preferred_element_type=jnp.float32)
            acc = part if acc is None else acc + part
            pre = jnp.dot(xb[0:3 * rows, :], win_ref[:, t], preferred_element_type=jnp.float32)
            for s in range(4):
                a = a0[0:rows, t] if s == 0 else pre[(s - 1) * rows:s * rows, :]
                v = a * scale[index[s], :, t] + shift[index[s], :, t]
                g = (v + v * jnp.tanh(v * (K1 * (v * v) + K0))).astype(jnp.bfloat16)
                if s < 3:
                    hid[s * rows:(s + 1) * rows, t] = g
                else:
                    term = h_row[index[s], :, 0:TILE] * g.astype(jnp.float32)
                    good = jnp.logical_and(steps[s] >= 0, steps[s] < STEPS)
                    total[0:rows, t] += jnp.where(good, term, 0.0)
        for s in range(3):
            j = n - 1 - s
            good = jnp.logical_and(j >= 0, j < STEPS)
            term = h_row[jnp.clip(j, 0, STEPS - 1)] * acc[s * rows:(s + 1) * rows, :]
            run[s, 0:rows] = run[s, 0:rows] + jnp.where(good, term, 0.0)

    for p in range(PASSES):
        rows = spans[p][1]
        run[...] = jnp.zeros_like(run)
        total[...] = jnp.zeros_like(total)
        hid[...] = jnp.zeros_like(hid)
        xb[0:rows, :] = x_s[pl.ds(*spans[p])].astype(jnp.bfloat16)
        for t in tiles:
            a0[0:rows, t] = jnp.dot(xb[0:rows, :], win_ref[:, t], preferred_element_type=jnp.float32)

        def block(b, carry, p=p):
            if p == 0:
                @pl.when(b + 2 == me)
                def _():
                    send_mods()

                take_mods(b)
            else:
                for at, stage in ((7, gather_second), (13, gather_third)):
                    @pl.when(b == at)
                    def _(stage=stage):
                        stage(p - 1)

            def inner(k, carry):
                body(p, b * OWN + k)
                return carry
            lax.fori_loop(0, OWN, inner, 0, unroll=OWN)
            return carry

        lax.fori_loop(0, DEVS, block, 0)
        if p > 0:
            gather_last(p - 1)

        def tail(k, carry, p=p):
            body(p, STEPS + k)
            return carry
        lax.fori_loop(0, 3, tail, 0, unroll=3)

        for t in tiles:
            rest = total[0:rows, t]
            for s in range(3):
                part = rest.astype(jnp.bfloat16)
                hid[s * rows:(s + 1) * rows, t] = part
                rest = rest - part.astype(jnp.float32)
        out = jnp.dot(hid[0:3 * rows, :], wout_ref[...], preferred_element_type=jnp.float32)
        out = out[0:rows] + (out[rows:2 * rows] + out[2 * rows:3 * rows])
        y_all[me, pl.ds(*spans[p])] = x_s[pl.ds(*spans[p])] + out
        gather_first(p)

    last = PASSES - 1
    gather_second(last)
    gather_third(last)
    gather_last(last)
    for p in range(PASSES):
        for d in range(1, 4):
            z_send(p, d).wait_send()
        for k in range(4):
            y_send(p, k).wait_send()
        for k in range(8):
            c_send(p, k).wait_send()

    def sent(d, carry):
        for copy in mod_copies(d, me, lax.rem(me + d, DEVS)):
            copy.wait_send()
        return carry
    lax.fori_loop(1, DEVS, sent, 0)
    for p in range(PASSES):
        out_copy(p).wait()


def solution(mesh):
    assert mesh.shape["time"] == DEVS

    def local_run(x_init, w_in, w_out, mod_gamma, mod_beta, step_size):
        channels, hidden = w_in.shape
        every = x_init.size // channels // DEVS
        rows = every * 2 // 3
        x_rows = x_init.reshape(DEVS, every, channels)
        h_wide = jnp.broadcast_to(step_size[:, None], (OWN, channels))
        vmem = pl.BlockSpec(memory_space=pltpu.VMEM)
        dma = pltpu.SemaphoreType.DMA
        f32, bf16 = jnp.float32, jnp.bfloat16
        y = pl.pallas_call(
            _sampler,
            out_shape=jax.ShapeDtypeStruct((DEVS, every, channels), f32),
            in_specs=[pl.BlockSpec(memory_space=pltpu.HBM)] * 3 + [vmem] * 3,
            out_specs=pl.BlockSpec(memory_space=pl.ANY),
            scratch_shapes=[
                pltpu.VMEM((channels, hidden), bf16),
                pltpu.VMEM((hidden, channels), bf16),
                pltpu.VMEM((every, channels), f32),
                pltpu.VMEM((DEVS, OWN, hidden), bf16),
                pltpu.VMEM((DEVS, OWN, hidden), bf16),
                pltpu.VMEM((DEVS, OWN, channels), f32),
                pltpu.VMEM((STEPS, 1, hidden), f32),
                pltpu.VMEM((STEPS, 1, hidden), f32),
                pltpu.VMEM((STEPS, 1, channels), f32),
                pltpu.VMEM((rows, hidden), f32),
                pltpu.VMEM((3, rows, channels), f32),
                pltpu.VMEM((rows, hidden), f32),
                pltpu.VMEM((3 * rows, channels), bf16),
                pltpu.VMEM((3 * rows, hidden), bf16),
                pltpu.VMEM((DEVS, every, channels), f32),
                dma(()), dma((2,)), dma((PASSES,)),
                dma((DEVS, 3)), dma((DEVS, 3)),
                dma((PASSES, 3)), dma((PASSES, 3)),
                dma((PASSES, 4)), dma((PASSES, 4)),
                dma((PASSES, 8)), dma((PASSES, 8)),
            ],
            compiler_params=pltpu.CompilerParams(
                collective_id=0, has_side_effects=True, vmem_limit_bytes=67_000_000),
            name="sampler",
        )(x_rows, w_in, w_out, mod_gamma, mod_beta, h_wide)
        return y.reshape(x_init.shape)

    return jax.shard_map(
        local_run, mesh=mesh,
        in_specs=(P("data", None, None), P(None, None), P(None, None),
                  P("time", None), P("time", None), P("time")),
        out_specs=P("data", None, None), check_vma=False)
```
